32 devices in a mesh: tm: 8 (over z, y), row: 2 (over core), col: 2 (over x).
Axes of the slice: x: 2, y: 2, z: 4, core: 2. Of those that a mesh axis runs over, the one named last changes fastest.
Arguments:
- precision_diag: float32 [16, 512, 512], P('tm', 'row', 'col'), may hold values from -4 to 16, as said below
- precision_link: float32 [16, 512, 512], P('tm', 'row', 'col'), may hold values from -8 to 2
Outputs:
- pivots: float32 [16, 512, 512], P('tm', 'row', 'col')
- couplings: float32 [16, 512, 512], P('tm', 'row', 'col')
- log_variance: float32 [16, 512], P('tm', ('row', 'col'))
The draws below stay inside these ranges and needn't reach their ends.
Inputs may be any that keep to these rules, and one draw needn't show every extreme that they name: precision_diag and precision_link form a symmetric positive definite block-tridiagonal matrix as in the reference program.
All inputs are finite; a program needn't handle non-finite values.
Results may differ from the reference program's by a relative error of at most 0.0003.
Values sent between devices are 32-bit elements; how exact they have to be, the bound alone decides.
A program may use at most 128 MiB of HBM per device.

```python
import math
import jax
import jax.numpy as jnp
from jax import lax

NS = 512
LEVELS = 4
NT = 16


def paired_product(left_stack, right_stack):
    return jnp.einsum('jki,jkl->jil', left_stack, right_stack, precision=lax.Precision.HIGHEST)


def build_precision(key):
    base_key = jax.random.fold_in(key, 11)
    subkeys = jax.random.split(base_key, 6)
    scales = jnp.exp(jax.random.uniform(subkeys[0], (NT, NS), jnp.float32, math.log(0.7), math.log(2.2)))
    identity = jnp.eye(NS, dtype=jnp.float32)
    roughness = jax.random.normal(subkeys[1], (NT, NS, NS), jnp.float32) * (0.5 / math.sqrt(NS))
    factor = jnp.triu(roughness, 1) + scales[:, :, None] * identity
    persistence = jax.random.uniform(subkeys[2], (NT,), jnp.float32, 0.985, 0.999)
    shocked = jax.random.uniform(subkeys[3], (NT,), jnp.float32) < 0.03
    persistence = jnp.where(shocked, 0.6, persistence)
    perturbation = jax.random.normal(subkeys[4], (NT, NS, NS), jnp.float32) * (0.1 / math.sqrt(NS))
    transfer = persistence[:, None, None] * (factor + perturbation)
    nugget = jnp.exp(jax.random.uniform(subkeys[5], (NT, NS), jnp.float32, math.log(0.0001), math.log(0.01))) * scales * scales
    next_factor = jnp.roll(factor, -1, axis=0)
    next_transfer = jnp.roll(transfer, -1, axis=0)
    present = (jnp.arange(NT) < NT - 1).astype(jnp.float32)[:, None, None]
    diagonal_blocks = paired_product(factor, factor) + present * paired_product(next_transfer, next_transfer) + nugget[:, :, None] * identity
    link_blocks = -paired_product(next_factor, next_transfer)
    return (diagonal_blocks, link_blocks)


def draw_precision_diag(key, part):
    return build_precision(key)[0]


def draw_precision_link(key, part):
    return build_precision(key)[1]


def setup_inputs(seed: int = 0) -> dict:
    key_list = jax.random.split(jax.random.key(seed), 3)
    precision_diag = draw_precision_diag(jax.random.fold_in(key_list[2], 71), 0)
    precision_link = draw_precision_link(jax.random.fold_in(key_list[2], 71), 0)
    return dict(precision_diag=precision_diag, precision_link=precision_link)


def product_tn(left_part, right_part):
    return jnp.einsum('ki,kl->il', left_part, right_part, precision=lax.Precision.HIGHEST)

def eliminate_block(pivot, below_link, above_link):
    node_count = pivot.shape[0]
    lower_factor = jnp.linalg.cholesky(pivot)
    right_side = jnp.concatenate([below_link, above_link.T, jnp.eye(node_count, dtype=pivot.dtype)], axis=1)
    solved = jax.scipy.linalg.solve_triangular(lower_factor, right_side, lower=True)
    lower_panel = solved[:, :node_count]
    upper_panel = solved[:, node_count:2 * node_count]
    inverse_part = solved[:, 2 * node_count:]
    log_part = jnp.log(jnp.sum(inverse_part * inverse_part, axis=0))
    return (log_part, product_tn(lower_panel, lower_panel), product_tn(upper_panel, upper_panel), -product_tn(upper_panel, lower_panel))

def final_block(pivot):
    node_count = pivot.shape[0]
    lower_factor = jnp.linalg.cholesky(pivot)
    inverse_part = jax.scipy.linalg.solve_triangular(lower_factor, jnp.eye(node_count, dtype=pivot.dtype), lower=True)
    return jnp.log(jnp.sum(inverse_part * inverse_part, axis=0))

def reference(precision_diag, precision_link):
    block_total = precision_diag.shape[0]
    node_count = precision_diag.shape[1]
    pivots = precision_diag
    links = precision_link.at[block_total - 1].set(jnp.zeros((node_count, node_count), precision_link.dtype))
    out_pivots = pivots
    out_links = links
    out_logs = jnp.zeros((block_total, node_count), precision_diag.dtype)
    for level_num in range(LEVELS):
        stride = 2 ** level_num
        removed = jnp.arange(stride, block_total, 2 * stride, dtype=jnp.int32)
        lower_ids = (removed - stride).astype(jnp.int32)
        upper_ids = (removed + stride).astype(jnp.int32)
        log_part, gram_down, gram_up, link_new = jax.vmap(eliminate_block)(pivots[removed], links[lower_ids], links[removed])
        out_pivots = out_pivots.at[removed].set(pivots[removed])
        out_links = out_links.at[removed].set(links[removed])
        out_logs = out_logs.at[removed].set(log_part)
        pivots = pivots.at[lower_ids].add(-gram_down)
        pivots = pivots.at[upper_ids].add(-gram_up, mode='drop')
        links = links.at[lower_ids].set(link_new)
    kept = jnp.arange(0, block_total, 2 ** LEVELS, dtype=jnp.int32)
    out_pivots = out_pivots.at[kept].set(pivots[kept])
    out_links = out_links.at[kept].set(links[kept])
    out_logs = out_logs.at[kept].set(jax.vmap(final_block)(pivots[kept]))
    return (out_pivots, out_links, out_logs)
```

```python
import jax
import jax.numpy as jnp
from jax import lax
from jax.experimental import pallas as pl
from jax.experimental.pallas import tpu as pltpu
from jax.sharding import PartitionSpec as P

LEVELS = 4

LANES = 128
ROWS = 8
GROUP = 32


def split_three(array):
    high = array.astype(jnp.bfloat16)
    rest = array - high.astype(jnp.float32)
    middle = rest.astype(jnp.bfloat16)
    return high, middle, (rest - middle.astype(jnp.float32)).astype(jnp.bfloat16)


def packed_dot(left, right):
    high, middle, low = split_three(left)
    first, second, third = split_three(right)
    wide = jnp.concatenate([high, high, middle, middle, high, low], axis=1)
    tall = jnp.concatenate([first, second, first, second, third, first], axis=0)
    return jnp.dot(wide, tall, preferred_element_type=jnp.float32)


def sweep_group(strips, start):
    sub = lax.broadcasted_iota(jnp.int32, (ROWS, LANES), 0)
    lane = lax.broadcasted_iota(jnp.int32, (ROWS, LANES), 1)
    pick = lambda strip, row: jnp.broadcast_to(strip[row : row + 1, :], (ROWS, LANES))
    strips = list(strips)
    count = len(strips)

    def spread(strip, p):
        return [
            jnp.broadcast_to(strip[:, start + ROWS * p + j : start + ROWS * p + j + 1], (ROWS, LANES)) for j in range(ROWS)
        ]

    def total(terms):
        while len(terms) > 1:
            terms = [terms[m] + terms[m + 1] for m in range(0, len(terms), 2)]
        return terms[0]

    cols = spread(strips[0], 0)
    for p in range(count):
        base = start + ROWS * p
        inside = (lane >= base) & (lane < base + ROWS)
        panel = jnp.where(inside, jnp.where(lane - base == sub, 1.0, 0.0), strips[p])
        if p + 1 < count:
            ahead_cols = spread(strips[p], p + 1)
            next_left = spread(strips[p + 1], p)
            next_cols = spread(strips[p + 1], p + 1)
        for i in range(0, ROWS, 2):
            first, second = cols[i], cols[i + 1]
            on_first, on_second = sub == i, sub == i + 1
            outside = (sub < i) | (sub > i + 1)
            a, b = pick(first, i), pick(first, i + 1)
            d = pick(second, i + 1)
            det = a * d - b * b
            scale = pl.reciprocal(det, approx=True)
            left = jnp.where(on_first, d, jnp.where(on_second, -b, second * b - first * d))
            right = jnp.where(on_second, a, jnp.where(on_first, -b, first * b - second * a))
            scale = scale * (2.0 - det * scale)
            apply = lambda strip: jnp.where(outside, strip, 0.0) + scale * (left * pick(strip, i) + right * pick(strip, i + 1))
            panel = apply(panel)
            for j in range(i + 2, ROWS):
                cols[j] = apply(cols[j])
            if p + 1 < count:
                ahead_cols = [apply(strip) for strip in ahead_cols]
        if p + 1 < count:
            cols = [
                next_cols[j] - total([next_left[m] * pick(ahead_cols[j], m) for m in range(ROWS)])
                for j in range(ROWS)
            ]
        for q in [q for q in range(p + 1, count)] + [q for q in range(p)]:
            left_cols = next_left if q == p + 1 else spread(strips[q], p)
            strips[q] = jnp.where(inside, 0.0, strips[q]) - total(
                [c * pick(panel, j) for j, c in enumerate(left_cols)]
            )
        strips[p] = panel
    return strips


def split_two(array):
    high = array.astype(jnp.bfloat16)
    return high, (array - high.astype(jnp.float32)).astype(jnp.bfloat16)


def wide_left(array):
    high, low = split_two(array)
    return jnp.concatenate([high, high, low], axis=1)


def wide_right(array):
    high, low = split_two(array)
    return jnp.concatenate([high, low, high], axis=1)


def tall_right(array):
    high, low = split_two(array)
    return jnp.concatenate([high, low, high], axis=0)


def mul(wide, tall):
    return jnp.dot(wide, tall, preferred_element_type=jnp.float32)


def mul_nt(wide, other):
    return lax.dot_general(wide, other, (((1,), (1,)), ((), ())), preferred_element_type=jnp.float32)


def invert_lanes(block, middle):
    lane = lax.broadcasted_iota(jnp.int32, (LANES, LANES), 1)
    for start in range(0, LANES, GROUP):
        if start == LANES // 2:
            middle()
        strips = [block[start + ROWS * q : start + ROWS * (q + 1), :] for q in range(GROUP // ROWS)]
        solved = sweep_group(strips, start)
        inside = (lane >= start) & (lane < start + GROUP)
        above = [jnp.zeros((start, LANES), jnp.float32)] if start else []
        rest = LANES - start - GROUP
        below = [jnp.zeros((rest, LANES), jnp.float32)] if rest else []
        padded = jnp.concatenate(above + solved + below, axis=0)
        update = packed_dot(jnp.where(inside, block, 0.0), padded)
        block = jnp.where(inside, 0.0, block) - update
        block = jnp.concatenate(
            ([block[:start, :]] if start else []) + solved + ([block[start + GROUP :, :]] if rest else []), axis=0
        )
    return block


def sweep_ref(work, before, middle, after):
    node_count = work.shape[0]

    def step(k, carry):
        before(k)
        here = pl.ds(pl.multiple_of(k * LANES, LANES), LANES)
        inverse = invert_lanes(work[here, here], lambda: middle(k))
        after(k)
        row_block = lax.broadcasted_iota(jnp.int32, (node_count, LANES), 0) // LANES
        column = jnp.where(row_block == k, 0.0, work[:, here])
        wide = wide_right(column)
        solved = mul(wide_left(column), tall_right(inverse))
        across = mul_nt(wide_left(inverse), wide)
        work[...] = work[...] - mul_nt(wide_left(solved), wide)
        work[:, here] = solved
        work[here, :] = across
        work[here, here] = -inverse
        return carry

    lax.fori_loop(0, node_count // LANES, step, 0)


def cyclic_kernel(
    diag_ref, link_ref, pivot_ref, coupling_ref, log_ref,
    base, links, work, solved, packed, landed, final, link_out, base_out, home_tiles, log_out, home_log,
    dx_send, dx_recv, dr_send, dr_recv, df_send, df_recv,
    lx_send, lx_recv, lr_send, lr_recv, lf_send, lf_recv,
    up_send, up_recv, pass_send, pass_recv, link_send, link_recv, base_send, base_recv, home_send, home_recv,
):
    time_id, row_id, col_id = lax.axis_index("tm"), lax.axis_index("row"), lax.axis_index("col")
    times = lax.axis_size("tm")
    half = diag_ref.shape[1]
    chunk = half // 2
    node_count = 2 * half
    blocks = node_count // LANES
    reach = LEVELS - 1
    mesh_id = pl.DeviceIdType.MESH
    power = lambda p: sum(jnp.where(p == j, 2**j, 0) for j in range(LEVELS))
    depth = sum((lax.rem(time_id + 1, 2**j) == 0).astype(jnp.int32) for j in range(1, LEVELS))
    keeps_all = depth == reach
    phases = depth + 1 + keeps_all.astype(jnp.int32)
    mine = jnp.where(row_id == col_id, 0, 1)
    leads = mine == 0
    low, high = pl.ds(0, half), pl.ds(half, half)
    part = lambda index: pl.ds(pl.multiple_of(index * half, LANES), half)
    ours = part(mine)
    starts = [sum(node_count - LANES * i for i in range(j)) for j in range(blocks + 1)]
    strip = (node_count - LANES) // 2
    rest = (starts[blocks] - starts[2]) // 2

    def copy(src, dst, send, recv, target):
        return pltpu.make_async_remote_copy(
            src_ref=src, dst_ref=dst, send_sem=send, recv_sem=recv, device_id=target, device_id_type=mesh_id
        )

    sibling, across_x = {"row": 1 - row_id}, {"col": 1 - col_id}

    level_of = 1 + sum((lax.rem(time_id, 2**j) == 0).astype(jnp.int32) for j in range(1, LEVELS))
    is_home = level_of > 1
    home_from = time_id + power(level_of - 1) - 1
    edges = [(time_id + power(depth), time_id + power(depth) < times)]
    for p in range(LEVELS):
        below = (p < depth) | (keeps_all & (p == reach))
        edges.append((time_id - 2**p, below & (time_id >= 2**p)))
    for p in range(2, LEVELS + 1):
        edges.append((time_id + 1 - 2 ** (p - 1), p < phases))
    edges.append((home_from, is_home))

    barrier = pltpu.get_barrier_semaphore()
    pl.semaphore_signal(barrier, inc=1, device_id=sibling, device_id_type=mesh_id)
    pl.semaphore_signal(barrier, inc=1, device_id=across_x, device_id_type=mesh_id)
    greeted = 2
    for other, near in edges:
        @pl.when(near)
        def _(other=other):
            pl.semaphore_signal(barrier, inc=1, device_id={"tm": other}, device_id_type=mesh_id)

        greeted = greeted + near.astype(jnp.int32)
    pl.semaphore_wait(barrier, greeted)

    def dx_copy(ph):
        return copy(base.at[ph, ours, low], base.at[ph, part(1 - mine), high], dx_send.at[ph], dx_recv.at[ph], across_x)

    def dx_arrival(ph):
        tile = base.at[ph, ours, high]
        return copy(tile, tile, dx_send.at[ph], dx_recv.at[ph], across_x)

    def dr_copy(ph):
        tile = base.at[ph, ours, low]
        return copy(tile, tile, dr_send.at[ph], dr_recv.at[ph], sibling)

    def df_copy(ph):
        tile = base.at[ph, high, high]
        return copy(tile, tile, df_send.at[ph], df_recv.at[ph], sibling)

    def start_base(ph):
        dr_copy(ph).start()

        @pl.when(leads)
        def _():
            dx_copy(ph).start()

    def link_tile(ph, slot, j, where):
        turned = (ph == 0) if slot == 0 else False
        own = jnp.where(turned, 0, mine * half) + j * chunk, jnp.where(turned, mine * half, 0)
        away = jnp.where(turned, half, (1 - mine) * half) + j * chunk, jnp.where(turned, (1 - mine) * half, half)
        got = jnp.where(turned, half, mine * half) + j * chunk, jnp.where(turned, mine * half, half)
        row, col = {"own": own, "away": away, "got": got}[where]
        return links.at[ph, slot, pl.ds(pl.multiple_of(row, LANES), chunk), pl.ds(pl.multiple_of(col, LANES), half)]

    def lx_copy(ph, slot, j):
        sems = lx_send.at[ph, slot, j], lx_recv.at[ph, slot, j]
        return copy(link_tile(ph, slot, j, "own"), link_tile(ph, slot, j, "away"), *sems, across_x)

    def lx_arrival(ph, slot, j):
        tile = link_tile(ph, slot, j, "got")
        return copy(tile, tile, lx_send.at[ph, slot, j], lx_recv.at[ph, slot, j], across_x)

    def lr_copy(ph, slot, j):
        tile = link_tile(ph, slot, j, "own")
        return copy(tile, tile, lr_send.at[ph, slot, j], lr_recv.at[ph, slot, j], sibling)

    def lf_copy(ph, slot, j):
        tile = link_tile(ph, slot, j, "got")
        return copy(tile, tile, lf_send.at[ph, slot, j], lf_recv.at[ph, slot, j], sibling)

    def start_link(ph, slot, j):
        lx_copy(ph, slot, j).start()
        lr_copy(ph, slot, j).start()

    def pass_link(ph, slot, j):
        lx_arrival(ph, slot, j).wait_recv()
        lf_copy(ph, slot, j).start()

    def end_link(ph, slot, j):
        lr_copy(ph, slot, j).wait_recv()
        lf_copy(ph, slot, j).wait_recv()

    def piece(i):
        if i == 0:
            return pl.ds(0, LANES)
        first, size = ((LANES, strip), (starts[1], strip), (starts[2], rest))[i - 1]
        if i == 2:
            size = (starts[2] - starts[1]) // 2
        return pl.ds(pl.multiple_of(first + row_id * size, 8), size)

    def up_copy(p, i):
        return copy(packed.at[1, piece(i)], landed.at[p, piece(i)], up_send.at[i], up_recv.at[p, i], {"tm": time_id + power(p)})

    def pass_copy(p, i):
        tile = landed.at[p, piece(i)]
        return copy(tile, tile, pass_send.at[p, i], pass_recv.at[p, i], sibling)

    def link_copy(p, j):
        rows = pl.ds(pl.multiple_of(mine * half + j * chunk, LANES), chunk)
        return copy(
            link_out.at[pl.ds(j * chunk, chunk)], links.at[p + 1, 0, rows, low], link_send.at[j], link_recv.at[p, j],
            {"tm": time_id + power(p)},
        )

    def base_copy(p):
        return copy(base_out, base.at[p + 2, ours, low], base_send.at[0], base_recv.at[p], {"tm": time_id + power(p)})

    def home_copy(ph, i):
        src = (final.at[ph - 1, ours], links.at[ph, 1, ours, low], log_out.at[ph])[i]
        dst = (home_tiles.at[0], home_tiles.at[1], home_log)[i]
        return copy(src, dst, home_send.at[ph, i], home_recv.at[i], {"tm": time_id + 1 - power(ph - 1)})

    def phase(ph, carry):
        first = ph == 0
        later = ph > 0
        solving = ph < LEVELS
        keeper = solving & ((ph < depth) | keeps_all)
        sender = (ph == depth) & jnp.logical_not(keeps_all)
        below = jnp.maximum(ph - 1, 0)
        joined = later & (time_id >= power(below))

        @pl.when(first)
        def _():
            base[0, ours, low] = diag_ref[1]
            start_base(0)
            upper = jnp.where(time_id == times - 1, 0.0, link_ref[1])
            links[0, 1, ours, low] = upper
            for j in (0, 1):
                start_link(0, 1, j)
            links[0, 0, low, ours] = link_ref[0].T
            for j in (0, 1):
                start_link(0, 0, j)
            base[1, ours, low] = diag_ref[0]

            @pl.when(depth > 0)
            def _():
                start_base(1)

            pivot_ref[1] = diag_ref[1]
            coupling_ref[1] = upper
            packed[0] = jnp.zeros(packed.shape[1:], jnp.float32)

        work[...] = jnp.zeros(work.shape, jnp.float32)
        dr_copy(ph).wait_recv()

        @pl.when(joined)
        def _():
            up_copy(below, 0).wait_recv()

        def absorb(j, top, bottom):
            cols = slice(LANES * j, LANES * (j + 1))
            rows = slice(top, bottom)
            lines = slice(starts[j] + top - LANES * j, starts[j] + bottom - LANES * j)
            value = base[ph, rows, cols] + packed[0, lines]
            work[rows, cols] = work[rows, cols] + value
            shown = LANES * j < half
            if shown:
                @pl.when(later)
                def _():
                    final[below, rows, cols] = value

            @pl.when(joined)
            def _():
                extra = landed[below, lines]
                work[rows, cols] = work[rows, cols] + extra
                if shown:
                    final[below, rows, cols] = value + extra

        def before(k):
            for j in range(blocks):
                @pl.when(k == j)
                def _(j=j):
                    if j in (1, 2):
                        @pl.when(joined)
                        def _():
                            pass_copy(below, j + 1).wait_recv()
                    if j == blocks // 2:
                        @pl.when(leads)
                        def _():
                            df_copy(ph).wait_recv()
                    if j == blocks - 1:
                        @pl.when(later & solving)
                        def _():
                            link_copy(below, 1).wait_recv()
                            start_link(ph, 0, 1)
                    absorb(j, LANES * j, node_count if j else LANES)

        def middle(k):
            @pl.when((k == 0) & joined)
            def _():
                up_copy(below, 1).wait_recv()
                pass_copy(below, 1).start()

            @pl.when(k == 1)
            def _():
                @pl.when(joined)
                def _():
                    up_copy(below, 3).wait_recv()
                    pass_copy(below, 3).start()

                @pl.when(jnp.logical_not(leads))
                def _():
                    dx_arrival(ph).wait_recv()
                    df_copy(ph).start()

            @pl.when(k == 2)
            def _():
                @pl.when(first)
                def _():
                    for j in (0, 1):
                        pass_link(0, 1, j)

                @pl.when(later & solving)
                def _():
                    link_copy(below, 0).wait_recv()
                    start_link(ph, 0, 0)

                @pl.when(later)
                def _():
                    @pl.when(leads)
                    def _():
                        for i in range(half // LANES):
                            for j in range(i + 1, half // LANES):
                                upper, lower = slice(LANES * i, LANES * (i + 1)), slice(LANES * j, LANES * (j + 1))
                                final[below, upper, lower] = final[below, lower, upper].T

                    @pl.when(ph == 1)
                    def _():
                        pivot_ref[0] = final[0, ours]
                        coupling_ref[0] = links[1, 1, ours, low]

                    @pl.when(ph > 1)
                    def _():
                        home_copy(ph, 0).start()
                        home_copy(ph, 1).start()

            @pl.when((k == 3) & solving)
            def _():
                pass_link(ph, 0, 0)

        def after(k):
            @pl.when(k == 0)
            def _():
                @pl.when(joined)
                def _():
                    pass_copy(below, 1).wait_recv()

                absorb(0, LANES, node_count)

                @pl.when(joined)
                def _():
                    up_copy(below, 2).wait_recv()
                    pass_copy(below, 2).start()

        sweep_ref(work, before, middle, after)

        spot = pl.ds(pl.multiple_of(mine * half + col_id * (node_count // 4), LANES), node_count // 4)
        corner = work[spot, spot]
        same = lax.broadcasted_iota(jnp.int32, corner.shape, 0) == lax.broadcasted_iota(jnp.int32, corner.shape, 1)
        logs = jnp.log(-jnp.sum(jnp.where(same, corner, 0.0), axis=0, keepdims=True))

        @pl.when(ph < 2)
        def _():
            log_ref[pl.ds(1 - ph, 1), :] = logs

        @pl.when(ph > 1)
        def _():
            log_out[ph] = jnp.broadcast_to(logs, log_out.shape[1:])
            home_copy(ph, 2).start()

        @pl.when(solving)
        def _():
            pass_link(ph, 0, 1)

            @pl.when(first)
            def _():
                for j in (0, 1):
                    end_link(0, 1, j)

            for j in (0, 1):
                end_link(ph, 0, j)
            near, far = jnp.where(keeper, 0, 1), jnp.where(keeper, 1, 0)
            inverse = tall_right(work[...])
            left = wide_left(links[ph, near])
            solved[...] = mul(left, inverse)

            def panel(j):
                return mul_nt(left[LANES * j :, :], wide_right(solved[LANES * j : LANES * (j + 1), :]))

            def add_up(j, value):
                lines = slice(starts[j], starts[j + 1])

                @pl.when(first)
                def _():
                    packed[1, lines] = value

                @pl.when(later)
                def _():
                    packed[1, lines] = packed[1, lines] + value

            @pl.when(keeper)
            def _():
                for j in range(blocks):
                    packed[0, starts[j] : starts[j + 1]] = panel(j)

                @pl.when(later)
                def _():
                    base_copy(below).wait_recv()
                    start_base(ph + 1)

                other = wide_left(links[ph, 1])
                links[ph + 1, 1] = mul_nt(other, wide_right(solved[...]))

                @pl.when(time_id + 1 < times)
                def _():
                    solved[...] = mul(other, inverse)
                    for j in range(blocks):
                        value = mul_nt(other[LANES * j :, :], wide_right(solved[LANES * j : LANES * (j + 1), :]))
                        add_up(j, value)

                @pl.when((ph == reach) & (time_id + power(reach) < times))
                def _():
                    for i in range(4):
                        up_copy(reach, i).start()

            @pl.when(sender)
            def _():
                for j in range(blocks):
                    add_up(j, panel(j))
                    if j == 0:
                        up_copy(ph, 0).start()
                        up_copy(ph, 1).start()
                    if j == 1:
                        up_copy(ph, 2).start()
                up_copy(ph, 3).start()
                other = wide_left(links[ph, 0, ours])
                link_out[...] = mul_nt(other, wide_right(solved[0:half, :]))
                for j in (0, 1):
                    link_copy(ph, j).start()

                @pl.when(later)
                def _():
                    base_copy(below).wait_recv()

                reached = mul(wide_left(links[ph, 0, low]), inverse)
                base_out[...] = base[ph + 1, ours, low] + mul_nt(other, wide_right(reached))
                base_copy(ph).start()

        return carry

    lax.fori_loop(0, phases, phase, 0)

    @pl.when(is_home)
    def _():
        for i in range(3):
            home_copy(2, i).wait_recv()
        pivot_ref[0] = home_tiles[0]
        coupling_ref[0] = home_tiles[1]
        log_ref[0:1, :] = home_log[0:1, :]

    def drain(ph, carry):
        below = jnp.maximum(ph - 1, 0)
        dr = (ph > 0) | (ph == 0)
        dr_copy(ph).wait_send()

        @pl.when(leads)
        def _():
            dx_copy(ph).wait_send()

        @pl.when(jnp.logical_not(leads))
        def _():
            df_copy(ph).wait_send()

        def link_sends(slot):
            for j in (0, 1):
                lx_copy(ph, slot, j).wait_send()
                lr_copy(ph, slot, j).wait_send()
                lf_copy(ph, slot, j).wait_send()

        @pl.when(ph < LEVELS)
        def _():
            link_sends(0)

        @pl.when(ph == 0)
        def _():
            link_sends(1)

        @pl.when((ph > 0) & (time_id >= power(below)))
        def _():
            for i in (1, 2, 3):
                pass_copy(below, i).wait_send()

        @pl.when(ph > 1)
        def _():
            for i in range(3):
                home_copy(ph, i).wait_send()

        return carry

    lax.fori_loop(0, phases, drain, 0)

    @pl.when(time_id + power(depth) < times)
    def _():
        for i in range(4):
            up_copy(depth, i).wait_send()

    @pl.when(depth < reach)
    def _():
        for j in (0, 1):
            link_copy(depth, j).wait_send()
        base_copy(depth).wait_send()


def shards(precision_diag, precision_link):
    half = precision_diag.shape[1]
    node_count = 2 * half
    blocks = node_count // LANES
    lines = LANES * LANES // LANES * blocks * (blocks + 1) // 2
    vmem = pl.BlockSpec(memory_space=pltpu.VMEM)
    dma = pltpu.SemaphoreType.DMA
    real = lambda *shape: pltpu.VMEM(shape, jnp.float32)
    stack = jax.ShapeDtypeStruct(precision_diag.shape, jnp.float32)
    phases = LEVELS + 1
    pair = (LEVELS, 2, 2)
    return pl.pallas_call(
        cyclic_kernel,
        out_shape=(stack, stack, jax.ShapeDtypeStruct((2, node_count // 4), jnp.float32)),
        in_specs=[vmem, vmem],
        out_specs=(vmem, vmem, vmem),
        scratch_shapes=[
            real(phases, node_count, node_count),
            real(phases, 2, node_count, node_count),
            real(node_count, node_count),
            real(node_count, node_count),
            real(2, lines, LANES),
            real(LEVELS, lines, LANES),
            real(LEVELS, node_count, half),
            real(half, half),
            real(half, half),
            real(2, half, half),
            real(phases, ROWS, node_count // 4),
            real(ROWS, node_count // 4),
            dma((phases,)), dma((phases,)), dma((phases,)), dma((phases,)), dma((phases,)), dma((phases,)),
            dma(pair), dma(pair), dma(pair), dma(pair), dma(pair), dma(pair),
            dma((4,)), dma((LEVELS, 4)), dma((LEVELS, 4)), dma((LEVELS, 4)),
            dma((2,)), dma((LEVELS, 2)), dma((1,)), dma((LEVELS,)), dma((phases, 3)), dma((3,)),
        ],
        compiler_params=pltpu.CompilerParams(collective_id=0, has_side_effects=True),
    )(precision_diag, precision_link)


def solution(mesh):
    in_specs = (P("tm", "row", "col"), P("tm", "row", "col"))
    out_specs = (P("tm", "row", "col"), P("tm", "row", "col"), P("tm", ("row", "col")))
    return jax.shard_map(shards, mesh=mesh, in_specs=in_specs, out_specs=out_specs, check_vma=False)
```

```python
import jax
import jax.numpy as jnp
from jax import lax
from jax.experimental import pallas as pl
from jax.experimental.pallas import tpu as pltpu
from jax.sharding import PartitionSpec as P

LEVELS = 4

LANES = 128
ROWS = 8
GROUP = 32
NEAR = 4


def sweep_group(strips, start):
    sub = lax.broadcasted_iota(jnp.int32, (ROWS, LANES), 0)
    lane = lax.broadcasted_iota(jnp.int32, (ROWS, LANES), 1)
    pick = lambda strip, row: jnp.broadcast_to(strip[row : row + 1, :], (ROWS, LANES))
    strips = list(strips)
    count = len(strips)
    zero = strips[0] * 0.0

    def spread(strip, p, columns):
        base = start + ROWS * p
        return [jnp.broadcast_to(strip[:, base + j : base + j + 1], (ROWS, LANES)) + zero for j in columns]

    def total(terms):
        while len(terms) > 1:
            terms = [terms[m] + terms[m + 1] for m in range(0, len(terms), 2)]
        return terms[0]

    near, far = range(NEAR), range(NEAR, ROWS)
    cols = spread(strips[0], 0, range(ROWS))
    for p in range(count):
        base = start + ROWS * p
        inside = (lane >= base) & (lane < base + ROWS)
        panel = jnp.where(inside, jnp.where(lane - base == sub, 1.0, 0.0), strips[p])
        if p + 1 < count:
            ahead = spread(strips[p], p + 1, near)
            next_left = spread(strips[p + 1], p, range(ROWS))
            next_near = spread(strips[p + 1], p + 1, near)
        for i in range(0, ROWS, 2):
            first, second = cols[i], cols[i + 1]
            on_first, on_second = sub == i, sub == i + 1
            outside = (sub < i) | (sub > i + 1)
            a, b = pick(first, i), pick(first, i + 1)
            d = pick(second, i + 1)
            det = a * d - b * b
            scale = pl.reciprocal(det, approx=True)
            left = jnp.where(on_first, d, jnp.where(on_second, -b, second * b - first * d))
            right = jnp.where(on_second, a, jnp.where(on_first, -b, first * b - second * a))
            scale = scale * (2.0 - det * scale)
            left_scaled, right_scaled = scale * left, scale * right

            def soon(strip):
                return jnp.where(outside, strip, 0.0) + scale * (left * pick(strip, i) + right * pick(strip, i + 1))

            def apply(strip):
                return jnp.where(outside, strip, 0.0) + (left_scaled * pick(strip, i) + right_scaled * pick(strip, i + 1))

            for j in range(i + 2, ROWS):
                cols[j] = (soon if j < i + 4 else apply)(cols[j])
            last = i + 2 == ROWS
            panel = (soon if last else apply)(panel)
            if p + 1 < count:
                ahead = [(soon if last else apply)(strip) for strip in ahead]
        if p + 1 < count:
            cols = [next_near[j] - total([next_left[m] * pick(ahead[j], m) for m in range(ROWS)]) for j in near]
        rows = [pick(panel, j) for j in range(ROWS)]
        for q in [q for q in range(p + 1, count)] + [q for q in range(p)]:
            left_cols = next_left if q == p + 1 else spread(strips[q], p, range(ROWS))
            strips[q] = jnp.where(inside, 0.0, strips[q]) - total([c * rows[j] for j, c in enumerate(left_cols)])
            if q == p + 1:
                cols = cols + spread(strips[q], q, far)
        strips[p] = panel
    return strips


def split_two(array):
    high = array.astype(jnp.bfloat16)
    return high, (array - high.astype(jnp.float32)).astype(jnp.bfloat16)


def wide_left(array):
    high, low = split_two(array)
    return jnp.concatenate([high, high, low], axis=1)


def wide_right(array):
    high, low = split_two(array)
    return jnp.concatenate([high, low, high], axis=1)


def tall_right(array):
    high, low = split_two(array)
    return jnp.concatenate([high, low, high], axis=0)


def mul(wide, tall):
    return jnp.dot(wide, tall, preferred_element_type=jnp.float32)


def mul_nt(wide, other):
    return lax.dot_general(wide, other, (((1,), (1,)), ((), ())), preferred_element_type=jnp.float32)


def invert_lanes(block, middle=None, pause=LANES // 2):
    lane = lax.broadcasted_iota(jnp.int32, (LANES, LANES), 1)
    groups = LANES // GROUP
    for g in range(groups):
        start = GROUP * g
        if middle is not None and start == pause:
            middle()
        inside = (lane >= start) & (lane < start + GROUP)
        held = jnp.where(inside, block, 0.0)
        high = held.astype(jnp.bfloat16).astype(jnp.float32)
        low = held - high
        both = (high + pltpu.roll(low, GROUP, axis=1)).astype(jnp.bfloat16)
        twice = (both.astype(jnp.float32) + pltpu.roll(both.astype(jnp.float32), LANES // 2, axis=1)).astype(jnp.bfloat16)
        kept = jnp.where(inside, 0.0, block)
        strips = [block[start + ROWS * q : start + ROWS * (q + 1), :] for q in range(GROUP // ROWS)]
        solved = sweep_group(strips, start)
        first, second = split_two(jnp.concatenate(solved, axis=0))
        pieces = [None] * groups
        for at, value in enumerate((first, first, second, second)):
            pieces[(g + at) % groups] = value
        tall = jnp.concatenate(pieces, axis=0)
        bands = {g: jnp.concatenate(solved, axis=0)}
        order = [q for q in range(g + 1, groups)] + [q for q in range(g)]
        for q in order:
            rows = slice(GROUP * q, GROUP * (q + 1))
            bands[q] = kept[rows] - mul(twice[rows], tall)
        block = jnp.concatenate([bands[q] for q in range(groups)], axis=0)
    return block


def sweep_ref(work, pivot_ready, panel_ready, middle, prepare, early):
    node_count = work.shape[0]
    blocks = node_count // LANES
    span = lambda k: slice(LANES * k, LANES * (k + 1))
    late = LANES - GROUP
    pivot_ready(0)
    inverse = invert_lanes(work[span(0), span(0)], lambda: middle(0), late)
    for k in range(blocks):
        here = span(k)
        panel_ready(k)
        if k == blocks - 1:
            early(inverse)
        column = work[:, here]
        wide = wide_right(column)
        solved = mul(wide_left(column), tall_right(inverse))
        left = wide_left(solved)
        if k + 1 < blocks:
            pivot_ready(k + 1)
            ahead = span(k + 1)
            pivot = work[ahead, ahead] - mul_nt(left[ahead], wide[ahead])
        across = mul_nt(wide_left(inverse), wide)
        for j in range(blocks):
            if j == k:
                continue
            cols = span(j)
            pieces = [slice(0, LANES * k)] if k else []
            if j > k:
                top = LANES * (j + 1 if j == k + 1 else j)
                pieces += [slice(top, node_count)] if top < node_count else []
            for rows in pieces:
                work[rows, cols] = work[rows, cols] - mul_nt(left[rows], wide[cols])
            work[here, cols] = across[:, cols]
        if k:
            work[: LANES * k, here] = solved[: LANES * k]
        work[here, here] = -inverse
        if k + 2 < blocks:
            inverse = invert_lanes(pivot, lambda: middle(k + 1), late if k == 0 else LANES // 2)
        elif k + 1 < blocks:
            prepare()
            inverse = invert_lanes(pivot)


def cyclic_kernel(
    diag_ref, link_ref, pivot_ref, coupling_ref, log_ref,
    base, links, work, solved, packed, landed, final, link_out, base_out, home_tiles, log_out, home_log,
    part_sum, part_solved, last_panel, last_across, last_solved,
    dx_send, dx_recv, dr_send, dr_recv, df_send, df_recv,
    lx_send, lx_recv, lr_send, lr_recv, lf_send, lf_recv,
    up_send, up_recv, pass_send, pass_recv, link_send, link_recv, base_send, base_recv, home_send, home_recv,
):
    time_id, row_id, col_id = lax.axis_index("tm"), lax.axis_index("row"), lax.axis_index("col")
    times = lax.axis_size("tm")
    half = diag_ref.shape[1]
    chunk = half // 2
    node_count = 2 * half
    blocks = node_count // LANES
    reach = LEVELS - 1
    mesh_id = pl.DeviceIdType.MESH
    power = lambda p: sum(jnp.where(p == j, 2**j, 0) for j in range(LEVELS))
    depth = sum((lax.rem(time_id + 1, 2**j) == 0).astype(jnp.int32) for j in range(1, LEVELS))
    keeps_all = depth == reach
    phases = depth + 1 + keeps_all.astype(jnp.int32)
    mine = jnp.where(row_id == col_id, 0, 1)
    leads = mine == 0
    low, high = pl.ds(0, half), pl.ds(half, half)
    part = lambda index: pl.ds(pl.multiple_of(index * half, LANES), half)
    ours = part(mine)
    starts = [sum(node_count - LANES * i for i in range(j)) for j in range(blocks + 1)]
    bounds = [0, LANES, starts[1] + LANES, starts[2], starts[blocks]]
    heads, last = slice(0, node_count - LANES), slice(node_count - LANES, node_count)

    def copy(src, dst, send, recv, target):
        return pltpu.make_async_remote_copy(
            src_ref=src, dst_ref=dst, send_sem=send, recv_sem=recv, device_id=target, device_id_type=mesh_id
        )

    sibling, across_x = {"row": 1 - row_id}, {"col": 1 - col_id}

    level_of = 1 + sum((lax.rem(time_id, 2**j) == 0).astype(jnp.int32) for j in range(1, LEVELS))
    is_home = level_of > 1
    home_from = time_id + power(level_of - 1) - 1
    edges = [(time_id + power(depth), time_id + power(depth) < times)]
    for p in range(LEVELS):
        below = (p < depth) | (keeps_all & (p == reach))
        edges.append((time_id - 2**p, below & (time_id >= 2**p)))
    for p in range(2, LEVELS + 1):
        edges.append((time_id + 1 - 2 ** (p - 1), p < phases))
    edges.append((home_from, is_home))

    barrier = pltpu.get_barrier_semaphore()
    pl.semaphore_signal(barrier, inc=1, device_id=sibling, device_id_type=mesh_id)
    pl.semaphore_signal(barrier, inc=1, device_id=across_x, device_id_type=mesh_id)
    greeted = 2
    for other, near in edges:
        @pl.when(near)
        def _(other=other):
            pl.semaphore_signal(barrier, inc=1, device_id={"tm": other}, device_id_type=mesh_id)

        greeted = greeted + near.astype(jnp.int32)
    pl.semaphore_wait(barrier, greeted)

    def dx_copy(ph):
        return copy(base.at[ph, ours, low], base.at[ph, part(1 - mine), high], dx_send.at[ph], dx_recv.at[ph], across_x)

    def dx_arrival(ph):
        tile = base.at[ph, ours, high]
        return copy(tile, tile, dx_send.at[ph], dx_recv.at[ph], across_x)

    def dr_copy(ph):
        tile = base.at[ph, ours, low]
        return copy(tile, tile, dr_send.at[ph], dr_recv.at[ph], sibling)

    def df_copy(ph):
        tile = base.at[ph, high, high]
        return copy(tile, tile, df_send.at[ph], df_recv.at[ph], sibling)

    def start_base(ph):
        dr_copy(ph).start()

        @pl.when(leads)
        def _():
            dx_copy(ph).start()

    def link_tile(ph, slot, j, where):
        turned = (ph == 0) if slot == 0 else False
        own = jnp.where(turned, 0, mine * half) + j * chunk, jnp.where(turned, mine * half, 0)
        away = jnp.where(turned, half, (1 - mine) * half) + j * chunk, jnp.where(turned, (1 - mine) * half, half)
        got = jnp.where(turned, half, mine * half) + j * chunk, jnp.where(turned, mine * half, half)
        row, col = {"own": own, "away": away, "got": got}[where]
        return links.at[ph, slot, pl.ds(pl.multiple_of(row, LANES), chunk), pl.ds(pl.multiple_of(col, LANES), half)]

    def lx_copy(ph, slot, j):
        sems = lx_send.at[ph, slot, j], lx_recv.at[ph, slot, j]
        return copy(link_tile(ph, slot, j, "own"), link_tile(ph, slot, j, "away"), *sems, across_x)

    def lx_arrival(ph, slot, j):
        tile = link_tile(ph, slot, j, "got")
        return copy(tile, tile, lx_send.at[ph, slot, j], lx_recv.at[ph, slot, j], across_x)

    def lr_copy(ph, slot, j):
        tile = link_tile(ph, slot, j, "own")
        return copy(tile, tile, lr_send.at[ph, slot, j], lr_recv.at[ph, slot, j], sibling)

    def lf_copy(ph, slot, j):
        tile = link_tile(ph, slot, j, "got")
        return copy(tile, tile, lf_send.at[ph, slot, j], lf_recv.at[ph, slot, j], sibling)

    def start_link(ph, slot, j):
        lx_copy(ph, slot, j).start()
        lr_copy(ph, slot, j).start()

    def pass_link(ph, slot, j):
        lx_arrival(ph, slot, j).wait_recv()
        lf_copy(ph, slot, j).start()

    def end_link(ph, slot, j):
        lr_copy(ph, slot, j).wait_recv()
        lf_copy(ph, slot, j).wait_recv()

    def piece(i):
        if i == 0:
            return pl.ds(0, LANES)
        size = (bounds[i + 1] - bounds[i]) // 2
        return pl.ds(pl.multiple_of(bounds[i] + row_id * size, ROWS), size)

    def up_copy(p, i):
        return copy(packed.at[1, piece(i)], landed.at[p, piece(i)], up_send.at[i], up_recv.at[p, i], {"tm": time_id + power(p)})

    def pass_copy(p, i):
        tile = landed.at[p, piece(i)]
        return copy(tile, tile, pass_send.at[p, i], pass_recv.at[p, i], sibling)

    def link_copy(p, j):
        src = link_out.at[pl.ds(j * chunk, chunk)]
        dst = link_tile(p + 1, 0, j, "own") if j < 2 else link_tile(p + 1, 0, 0, "got")
        return copy(src, dst, link_send.at[j], link_recv.at[p, j], {"tm": time_id + power(p)})

    def base_copy(p):
        return copy(base_out, base.at[p + 2, ours, low], base_send.at[0], base_recv.at[p], {"tm": time_id + power(p)})

    def home_copy(ph, i):
        src = (final.at[ph - 1, ours], links.at[ph, 1, ours, low], log_out.at[ph])[i]
        dst = (home_tiles.at[0], home_tiles.at[1], home_log)[i]
        return copy(src, dst, home_send.at[ph, i], home_recv.at[i], {"tm": time_id + 1 - power(ph - 1)})

    def phase(ph, carry):
        first = ph == 0
        later = ph > 0
        solving = ph < LEVELS
        keeper = solving & ((ph < depth) | keeps_all)
        sender = (ph == depth) & jnp.logical_not(keeps_all)
        below = jnp.maximum(ph - 1, 0)
        joined = later & (time_id >= power(below))

        @pl.when(first)
        def _():
            base[0, ours, low] = diag_ref[1]
            start_base(0)
            upper = jnp.where(time_id == times - 1, 0.0, link_ref[1])
            links[0, 1, ours, low] = upper
            for j in (0, 1):
                start_link(0, 1, j)
            links[0, 0, low, ours] = link_ref[0].T
            for j in (0, 1):
                start_link(0, 0, j)
            base[1, ours, low] = diag_ref[0]

            @pl.when(depth > 0)
            def _():
                start_base(1)

            pivot_ref[1] = diag_ref[1]
            coupling_ref[1] = upper
            packed[...] = jnp.zeros(packed.shape, jnp.float32)

        work[...] = jnp.zeros(work.shape, jnp.float32)
        dr_copy(ph).wait_recv()

        @pl.when(joined)
        def _():
            up_copy(below, 0).wait_recv()

        def absorb(j, top, bottom):
            cols = slice(LANES * j, LANES * (j + 1))
            rows = slice(top, bottom)
            lines = slice(starts[j] + top - LANES * j, starts[j] + bottom - LANES * j)
            value = base[ph, rows, cols] + packed[0, lines]
            work[rows, cols] = work[rows, cols] + value
            shown = LANES * j < half
            if shown:
                @pl.when(later)
                def _():
                    final[below, rows, cols] = value

            @pl.when(joined)
            def _():
                extra = landed[below, lines]
                work[rows, cols] = work[rows, cols] + extra
                if shown:
                    final[below, rows, cols] = value + extra

        def pivot_ready(j):
            if j == 1:
                absorb(j, LANES, 2 * LANES)
                return
            if j == 2:
                @pl.when(joined)
                def _():
                    pass_copy(below, 3).wait_recv()
            if j == blocks // 2:
                @pl.when(leads)
                def _():
                    df_copy(ph).wait_recv()
            if j == blocks - 1:
                @pl.when(first)
                def _():
                    for i in (0, 1):
                        end_link(0, 1, i)

                @pl.when(later & solving)
                def _():
                    link_copy(below, 0).wait_recv()
                    lr_copy(ph, 0, 0).start()
            absorb(j, LANES * j, node_count if j else LANES)

        def panel_ready(j):
            if j == 0:
                @pl.when(joined)
                def _():
                    pass_copy(below, 1).wait_recv()

                absorb(0, LANES, node_count)
            if j == 1:
                @pl.when(joined)
                def _():
                    pass_copy(below, 2).wait_recv()

                absorb(1, 2 * LANES, node_count)

        def middle(k):
            if k == 0:
                @pl.when(joined)
                def _():
                    up_copy(below, 1).wait_recv()
                    pass_copy(below, 1).start()

            if k == 1:
                @pl.when(joined)
                def _():
                    for i in (2, 3):
                        up_copy(below, i).wait_recv()
                        pass_copy(below, i).start()

                @pl.when(jnp.logical_not(leads))
                def _():
                    dx_arrival(ph).wait_recv()
                    df_copy(ph).start()

            if k == 2:
                @pl.when(first)
                def _():
                    for j in (0, 1):
                        pass_link(0, 1, j)

                @pl.when(later & solving)
                def _():
                    link_copy(below, 1).wait_recv()
                    start_link(ph, 0, 1)

                @pl.when(later)
                def _():
                    @pl.when(leads)
                    def _():
                        for i in range(half // LANES):
                            for j in range(i + 1, half // LANES):
                                upper, lower = slice(LANES * i, LANES * (i + 1)), slice(LANES * j, LANES * (j + 1))
                                final[below, upper, lower] = final[below, lower, upper].T

                    @pl.when(ph == 1)
                    def _():
                        pivot_ref[0] = final[0, ours]
                        coupling_ref[0] = links[1, 1, ours, low]

                    @pl.when(ph > 1)
                    def _():
                        home_copy(ph, 0).start()
                        home_copy(ph, 1).start()

        def prepare():
            own = links[ph, 1]
            left = wide_left(own[:, heads])
            beside = work[heads, last]
            reached = mul(left, tall_right(work[heads, heads]))
            part_solved[...] = reached
            last_across[...] = beside
            last_panel[...] = own[:, last] - mul(left, tall_right(beside))
            for j in range(blocks):
                rows = slice(LANES * j, LANES * (j + 1))
                part_sum[starts[j] : starts[j + 1]] = mul_nt(left[LANES * j :], wide_right(reached[rows]))

        def add_up(inverse):
            ended = last_panel[...]
            wide = wide_right(ended)
            ahead = mul(wide_left(ended), tall_right(inverse))
            last_solved[...] = ahead
            left = wide_left(ahead)

            def add(j, top, bottom):
                lines = slice(starts[j] + top - LANES * j, starts[j] + bottom - LANES * j)
                value = part_sum[lines] - mul_nt(left[top:bottom], wide[LANES * j : LANES * (j + 1)])
                packed[1, lines] = packed[1, lines] + value

            return add

        def early(inverse):
            @pl.when(sender)
            def _():
                add = add_up(inverse)
                add(0, 0, LANES)
                up_copy(ph, 0).start()
                add(0, LANES, node_count)
                add(1, LANES, 2 * LANES)
                up_copy(ph, 1).start()
                add(1, 2 * LANES, node_count)
                up_copy(ph, 2).start()
                for j in range(2, blocks):
                    add(j, LANES * j, node_count)
                up_copy(ph, 3).start()

        sweep_ref(work, pivot_ready, panel_ready, middle, prepare, early)

        spot = pl.ds(pl.multiple_of(mine * half + col_id * (node_count // 4), LANES), node_count // 4)
        corner = work[spot, spot]
        same = lax.broadcasted_iota(jnp.int32, corner.shape, 0) == lax.broadcasted_iota(jnp.int32, corner.shape, 1)
        logs = jnp.log(-jnp.sum(jnp.where(same, corner, 0.0), axis=0, keepdims=True))

        @pl.when(ph < 2)
        def _():
            log_ref[pl.ds(1 - ph, 1), :] = logs

        @pl.when(ph > 1)
        def _():
            log_out[ph] = jnp.broadcast_to(logs, log_out.shape[1:])
            home_copy(ph, 2).start()

        def end_links():
            @pl.when(first)
            def _():
                pass_link(0, 0, 0)

            @pl.when(later)
            def _():
                link_copy(below, 2).wait_recv()
                lf_copy(ph, 0, 0).start()

            pass_link(ph, 0, 1)
            for j in (0, 1):
                end_link(ph, 0, j)

        @pl.when(keeper)
        def _():
            end_links()
            left = wide_left(links[ph, 0])
            solved[...] = mul(left, tall_right(work[...]))

            @pl.when(later)
            def _():
                base_copy(below).wait_recv()
                start_base(ph + 1)

            for j in range(blocks):
                rows = slice(LANES * j, LANES * (j + 1))
                packed[0, starts[j] : starts[j + 1]] = mul_nt(left[LANES * j :], wide_right(solved[rows]))
            links[ph + 1, 1] = mul_nt(wide_left(links[ph, 1]), wide_right(solved[...]))

            @pl.when(time_id + 1 < times)
            def _():
                add = add_up(-work[last, last])
                for j in range(blocks):
                    add(j, LANES * j, node_count)

            @pl.when((ph == reach) & (time_id + power(reach) < times))
            def _():
                for i in range(4):
                    up_copy(reach, i).start()

        @pl.when(sender)
        def _():
            end_links()
            ahead = last_solved[...]
            solved[:, heads] = part_solved[...] + mul_nt(wide_left(ahead), wide_right(last_across[...]))
            solved[:, last] = -ahead
            other = wide_left(links[ph, 0, ours])
            wide = wide_right(solved[...])
            link_out[chunk:half] = mul_nt(other[chunk:], wide[:half])
            link_copy(ph, 1).start()
            link_out[0:chunk] = mul_nt(other[:chunk], wide[:half])
            link_copy(ph, 0).start()
            link_out[half:] = mul_nt(other[:chunk], wide[half:])
            link_copy(ph, 2).start()

            @pl.when(later)
            def _():
                base_copy(below).wait_recv()

            reached = mul(wide_left(links[ph, 0, low]), tall_right(work[...]))
            base_out[...] = base[ph + 1, ours, low] + mul_nt(other, wide_right(reached))
            base_copy(ph).start()

        return carry

    lax.fori_loop(0, phases, phase, 0)

    @pl.when(is_home)
    def _():
        for i in range(3):
            home_copy(2, i).wait_recv()
        pivot_ref[0] = home_tiles[0]
        coupling_ref[0] = home_tiles[1]
        log_ref[0:1, :] = home_log[0:1, :]

    def drain(ph, carry):
        below = jnp.maximum(ph - 1, 0)
        dr_copy(ph).wait_send()

        @pl.when(leads)
        def _():
            dx_copy(ph).wait_send()

        @pl.when(jnp.logical_not(leads))
        def _():
            df_copy(ph).wait_send()

        def link_sends(slot):
            for j in (0, 1):
                @pl.when((ph == 0) | (j == 1))
                def _(j=j):
                    lx_copy(ph, slot, j).wait_send()

                lr_copy(ph, slot, j).wait_send()
                lf_copy(ph, slot, j).wait_send()

        @pl.when(ph < LEVELS)
        def _():
            link_sends(0)

        @pl.when(ph == 0)
        def _():
            link_sends(1)

        @pl.when((ph > 0) & (time_id >= power(below)))
        def _():
            for i in (1, 2, 3):
                pass_copy(below, i).wait_send()

        @pl.when(ph > 1)
        def _():
            for i in range(3):
                home_copy(ph, i).wait_send()

        return carry

    lax.fori_loop(0, phases, drain, 0)

    @pl.when(time_id + power(depth) < times)
    def _():
        for i in range(4):
            up_copy(depth, i).wait_send()

    @pl.when(depth < reach)
    def _():
        for j in range(3):
            link_copy(depth, j).wait_send()
        base_copy(depth).wait_send()


def shards(precision_diag, precision_link):
    half = precision_diag.shape[1]
    node_count = 2 * half
    blocks = node_count // LANES
    lines = LANES * blocks * (blocks + 1) // 2
    vmem = pl.BlockSpec(memory_space=pltpu.VMEM)
    dma = pltpu.SemaphoreType.DMA
    real = lambda *shape: pltpu.VMEM(shape, jnp.float32)
    stack = jax.ShapeDtypeStruct(precision_diag.shape, jnp.float32)
    phases = LEVELS + 1
    pair = (LEVELS, 2, 2)
    return pl.pallas_call(
        cyclic_kernel,
        out_shape=(stack, stack, jax.ShapeDtypeStruct((2, node_count // 4), jnp.float32)),
        in_specs=[vmem, vmem],
        out_specs=(vmem, vmem, vmem),
        scratch_shapes=[
            real(phases, node_count, node_count),
            real(phases, 2, node_count, node_count),
            real(node_count, node_count),
            real(node_count, node_count),
            real(2, lines, LANES),
            real(LEVELS, lines, LANES),
            real(LEVELS, node_count, half),
            real(half + half // 2, half),
            real(half, half),
            real(2, half, half),
            real(phases, ROWS, node_count // 4),
            real(ROWS, node_count // 4),
            real(lines, LANES),
            real(node_count, node_count - LANES),
            real(node_count, LANES),
            real(node_count - LANES, LANES),
            real(node_count, LANES),
            dma((phases,)), dma((phases,)), dma((phases,)), dma((phases,)), dma((phases,)), dma((phases,)),
            dma(pair), dma(pair), dma(pair), dma(pair), dma(pair), dma(pair),
            dma((4,)), dma((LEVELS, 4)), dma((LEVELS, 4)), dma((LEVELS, 4)),
            dma((3,)), dma((LEVELS, 3)), dma((1,)), dma((LEVELS,)), dma((phases, 3)), dma((3,)),
        ],
        compiler_params=pltpu.CompilerParams(collective_id=0, has_side_effects=True),
    )(precision_diag, precision_link)


def solution(mesh):
    in_specs = (P("tm", "row", "col"), P("tm", "row", "col"))
    out_specs = (P("tm", "row", "col"), P("tm", "row", "col"), P("tm", ("row", "col")))
    return jax.shard_map(shards, mesh=mesh, in_specs=in_specs, out_specs=out_specs, check_vma=False)
```
